32 devices in a mesh: data: 32 (over z, y, x, core).
Axes of the slice: x: 2, y: 2, z: 4, core: 2. Of those that a mesh axis runs over, the one named last changes fastest.
Arguments:
- x_now: bfloat16 [128, 197, 1024], P('data')
- x_next: bfloat16 [128, 197, 1024], P('data')
- labels: int32 [128], P('data')
- w_up: float32 [3, 1024, 4096], replicated
- w_down: float32 [3, 4096, 1024], replicated
- w_head: float32 [1024, 1000], replicated
- mom_up: float32 [3, 1024, 4096], P(None, None, 'data')
- mom_down: float32 [3, 4096, 1024], P(None, 'data')
- mom_head: float32 [1024, 1000], P('data')
- learn_rate: float32 [], replicated
- mom_decay: float32 [], replicated
Outputs:
- output 1: float32 [128, 1000], P('data')
- output 2: float32 [3, 1024, 4096], replicated
- output 3: float32 [3, 4096, 1024], replicated
- output 4: float32 [1024, 1000], replicated
- output 5: float32 [3, 1024, 4096], P(None, None, 'data')
- output 6: float32 [3, 4096, 1024], P(None, 'data')
- output 7: float32 [1024, 1000], P('data')
All inputs are finite; a program needn't handle non-finite values.
Results may differ from the reference program's by a relative error of at most 0.0189084.
Values are sent between devices in bfloat16 or wider.
A program may use at most 1 GiB of HBM per device.

```python
import math
import jax
import jax.numpy as jnp
from jax import lax

BATCH_DEV = 4
TOKENS = 197
WIDTH = 1024
HIDDEN = 4096
CLASSES = 1000
LAYERS = 3
GROUPS = 32
LN_EPS = 1e-6


def setup_inputs(seed: int = 0) -> dict:
    keys = jax.random.split(jax.random.key(seed), 13)
    batch = GROUPS * BATCH_DEV
    mom_scale = batch ** -0.5
    img_now = jax.random.normal(keys[0], (batch, 1, WIDTH), jnp.float32)
    tok_now = jax.random.normal(keys[1], (batch, TOKENS, WIDTH), jnp.float32)
    img_next = jax.random.normal(keys[2], (batch, 1, WIDTH), jnp.float32)
    tok_next = jax.random.normal(keys[3], (batch, TOKENS, WIDTH), jnp.float32)
    down_raw = jax.random.normal(keys[6], (LAYERS, HIDDEN, WIDTH), jnp.float32) * HIDDEN ** -0.5
    mom_raw = jax.random.normal(keys[9], (LAYERS, HIDDEN, WIDTH), jnp.float32) * (HIDDEN ** -0.5 * mom_scale)
    return {
        "x_now": (0.8 * img_now + 0.6 * tok_now).astype(jnp.bfloat16),
        "x_next": (0.8 * img_next + 0.6 * tok_next).astype(jnp.bfloat16),
        "labels": jax.random.randint(keys[4], (batch,), 0, CLASSES, jnp.int32),
        "w_up": jax.random.normal(keys[5], (LAYERS, WIDTH, HIDDEN), jnp.float32) * WIDTH ** -0.5,
        "w_down": down_raw - jnp.mean(down_raw, axis=1, keepdims=True),
        "w_head": jax.random.normal(keys[7], (WIDTH, CLASSES), jnp.float32) * WIDTH ** -0.5,
        "mom_up": jax.random.normal(keys[8], (LAYERS, WIDTH, HIDDEN), jnp.float32) * (WIDTH ** -0.5 * mom_scale),
        "mom_down": mom_raw - jnp.mean(mom_raw, axis=1, keepdims=True),
        "mom_head": jax.random.normal(keys[10], (WIDTH, CLASSES), jnp.float32) * (WIDTH ** -0.5 * mom_scale),
        "learn_rate": jax.random.uniform(keys[11], (), jnp.float32, 0.3, 0.6) * math.sqrt(batch),
        "mom_decay": jax.random.uniform(keys[12], (), jnp.float32, 0.7, 0.95),
    }


def norm_rows(values):
    mean_v = jnp.mean(values, axis=-1, keepdims=True)
    centered = values - mean_v
    var_v = jnp.mean(centered * centered, axis=-1, keepdims=True)
    return centered * lax.rsqrt(var_v + LN_EPS)


def block_fwd(x_rows, w_in, w_out):
    x_wide = x_rows.astype(jnp.float32)
    u_rows = norm_rows(x_wide).astype(jnp.bfloat16)
    pre_act = jnp.dot(u_rows, w_in.astype(jnp.bfloat16), preferred_element_type=jnp.float32).astype(jnp.bfloat16)
    gelu_out = jax.nn.gelu(pre_act.astype(jnp.float32), approximate=True).astype(jnp.bfloat16)
    block_out = jnp.dot(gelu_out, w_out.astype(jnp.bfloat16), preferred_element_type=jnp.float32).astype(jnp.bfloat16)
    return (x_wide + block_out.astype(jnp.float32)).astype(jnp.bfloat16)


def group_logits(x_grp, w_up, w_down, w_head):
    n_img, n_tok, width = x_grp.shape

    def layer_step(rows, layer_w):
        return block_fwd(rows, layer_w[0], layer_w[1]), None

    rows, _ = lax.scan(layer_step, x_grp.reshape(n_img * n_tok, width), (w_up, w_down))
    pooled = jnp.mean(rows.reshape(n_img, n_tok, width), axis=1, dtype=jnp.float32)
    normed = norm_rows(pooled).astype(jnp.bfloat16)
    return jnp.dot(normed, w_head.astype(jnp.bfloat16), preferred_element_type=jnp.float32)


def cross_ent(logits, labels):
    log_norm = jax.nn.logsumexp(logits, axis=-1)
    picked = jnp.sum(logits * jax.nn.one_hot(labels, logits.shape[-1], dtype=logits.dtype), axis=-1)
    return log_norm - picked


def reference(x_now, x_next, labels, w_up, w_down, w_head, mom_up, mom_down, mom_head, learn_rate, mom_decay):
    weights = (w_up, w_down, w_head)
    batch_total = GROUPS * BATCH_DEV
    x_groups = x_now.reshape(GROUPS, BATCH_DEV, TOKENS, WIDTH)
    label_groups = labels.reshape(GROUPS, BATCH_DEV)

    def accumulate(total, group):
        x_grp, lab_grp = group

        def group_loss(params):
            logits = group_logits(x_grp, params[0], params[1], params[2])
            return jnp.sum(cross_ent(logits, lab_grp)) / batch_total

        _, loss_pull = jax.vjp(group_loss, weights)
        gradients = loss_pull(jnp.ones((), jnp.float32))[0]
        return (total[0] + gradients[0], total[1] + gradients[1], total[2] + gradients[2]), None

    zero_grads = (jnp.zeros_like(w_up), jnp.zeros_like(w_down), jnp.zeros_like(w_head))
    gradients, _ = lax.scan(accumulate, zero_grads, (x_groups, label_groups))
    new_mom_up = mom_decay * mom_up + gradients[0]
    new_mom_down = mom_decay * mom_down + gradients[1]
    new_mom_head = mom_decay * mom_head + gradients[2]
    new_w_up = w_up - learn_rate * new_mom_up
    new_w_down = w_down - learn_rate * new_mom_down
    new_w_head = w_head - learn_rate * new_mom_head
    next_groups = x_next.reshape(GROUPS, BATCH_DEV, TOKENS, WIDTH)
    logits_next = lax.map(lambda x_grp: group_logits(x_grp, new_w_up, new_w_down, new_w_head), next_groups)
    logits_next = logits_next.reshape(GROUPS * BATCH_DEV, CLASSES)
    return (logits_next, new_w_up, new_w_down, new_w_head, new_mom_up, new_mom_down, new_mom_head)
```

```python
import functools

import jax
import jax.numpy as jnp
from jax import lax
from jax.experimental import pallas as pl
from jax.experimental.pallas import tpu as pltpu
from jax.sharding import PartitionSpec as P


LN_EPS = 1e-6
F32, BF16, I32 = jnp.float32, jnp.bfloat16, jnp.int32
LANES = 128
SUBS = 4
MASK = {"c": 1, "x": 2, "y": 4, "z0": 8, "z1": 16}
CONTRACT_LAST = (((1,), (1,)), ((), ()))
TANH_SCALE, TANH_CUBE = 0.7978845608028654, 0.044715
VMEM_LIMIT = 60 * 1024 * 1024

DOWN_LAST, UP_LAST = ("x", "y", "z0", "z1"), ("y", "x", "z0", "z1")
HALF_ORDERS = {(1, 1): ("z0", "x", "y"), (1, 0): ("x", "y", "z0"), (0, 1): ("y", "x", "z0"), (0, 0): ("z0", "y", "x")}
HEAD_ORDER = ("z0", "x", "y", "z1")
GATHER_SUB = {("up", 0): "x", ("down", 0): "y", ("up", 1): "z0", ("down", 1): "x", ("up", 2): "y", ("down", 2): "z0"}
GATHER_FIRST = {"x": ("z1", "z0", "y"), "y": ("z1", "z0", "x"), "z0": ("z1", "y", "x")}


def mm(lhs, rhs):
    return jnp.dot(lhs, rhs, preferred_element_type=F32)


def mm_t(lhs, rhs):
    return lax.dot_general(lhs, rhs, CONTRACT_LAST, preferred_element_type=F32)


def norm_parts(values):
    mean_v = jnp.mean(values, axis=-1, keepdims=True)
    centered = values - mean_v
    var_v = jnp.mean(centered * centered, axis=-1, keepdims=True)
    scale = lax.rsqrt(var_v + LN_EPS)
    return centered * scale, scale


def norm_rows(values):
    return norm_parts(values)[0]


def norm_grad(values, grad):
    normed, scale = norm_parts(values)
    inner = jnp.mean(grad * normed, axis=-1, keepdims=True)
    return scale * (grad - jnp.mean(grad, axis=-1, keepdims=True) - normed * inner)


def tanh_of(values):
    return jnp.tanh(TANH_SCALE * (values + TANH_CUBE * (values * values * values)))


def gelu(values):
    return values * (0.5 * (1.0 + tanh_of(values)))


def gelu_and_slope(values):
    t = tanh_of(values)
    half = 0.5 * (1.0 + t)
    slope = half + (0.5 * values) * ((1.0 - t * t) * (TANH_SCALE * (1.0 + (3.0 * TANH_CUBE) * (values * values))))
    return values * half, slope


def transposed(values, rows):
    depth, width = values.shape
    if rows > depth:
        values = jnp.concatenate([values, jnp.zeros((rows - depth, width), values.dtype)], axis=0)
    return values.astype(F32).T.astype(BF16)


def fold_rows(values):
    rows, width = values.shape
    return jnp.sum(values.reshape(rows // 8, 8, width), axis=0)


def side_by_side(refs, axis):
    return jnp.concatenate([r[0].astype(BF16) for r in refs], axis=axis)


def cost(flops, moved, trans=0):
    return pl.CostEstimate(flops=int(flops), bytes_accessed=int(moved), transcendentals=int(trans))


def params():
    return pltpu.CompilerParams(vmem_limit_bytes=VMEM_LIMIT)


def forward_kernel(tbl, x_ref, *refs):
    wu, wd = refs[0:4], refs[4:8]
    a_ref, xs_ref, ut_ref, zs_ref, pool_ref, u_s, z_s, x_s, acc = refs[8:]
    layer, j = pl.program_id(0), pl.program_id(1)
    last_layer, last_tile = pl.num_programs(0) - 1, pl.num_programs(1) - 1

    @pl.when((layer == 0) & (j == 0))
    def _():
        x_s[...] = x_ref[...]

    @pl.when(j == 0)
    def _():
        x_in = x_s[...]
        xs_ref[0] = x_in
        u = norm_rows(x_in.astype(F32)).astype(BF16)
        u_s[...] = u
        ut_ref[0] = transposed(u, ut_ref.shape[2])
        acc[...] = jnp.zeros_like(acc)

    a = mm(u_s[...], side_by_side(wu, 1)).astype(BF16)
    a_ref[0, 0] = a
    z = gelu(a.astype(F32)).astype(BF16)
    z_s[...] = z
    acc[...] += mm(z, side_by_side(wd, 0))

    @pl.when(layer == last_layer)
    def _():
        zs_ref[0, 0] = fold_rows(z_s[...].astype(F32))

    @pl.when(j == last_tile)
    def _():
        y = acc[...].astype(BF16)
        x_new = (x_s[...].astype(F32) + y.astype(F32)).astype(BF16)
        x_s[...] = x_new

        @pl.when(layer == last_layer)
        def _():
            pool_ref[...] = fold_rows(x_new.astype(F32))


def forward_now(tbl, x_rows, w_up, w_down, kept_rows):
    layers, width, hidden = w_up.shape
    rows = x_rows.shape[0]
    tiles = hidden // (LANES * SUBS)
    cols = LANES * SUBS

    def up_spec(i):
        return pl.BlockSpec((1, width, LANES), lambda l, j, t: (l, 0, t[j * SUBS + i]))

    def down_spec(i):
        return pl.BlockSpec((1, LANES, width), lambda l, j, t: (l, t[j * SUBS + i], 0))

    return pl.pallas_call(
        forward_kernel,
        grid_spec=pltpu.PrefetchScalarGridSpec(
            num_scalar_prefetch=1,
            grid=(layers, tiles),
            in_specs=[pl.BlockSpec((rows, width), lambda l, j, t: (0, 0))] + [up_spec(i) for i in range(SUBS)] + [down_spec(i) for i in range(SUBS)],
            out_specs=[
                pl.BlockSpec((1, 1, rows, cols), lambda l, j, t: (l, j, 0, 0)),
                pl.BlockSpec((1, rows, width), lambda l, j, t: (l, 0, 0)),
                pl.BlockSpec((1, width, kept_rows), lambda l, j, t: (l, 0, 0)),
                pl.BlockSpec((1, 1, 8, cols), lambda l, j, t: (l, j, 0, 0)),
                pl.BlockSpec((8, width), lambda l, j, t: (0, 0)),
            ],
            scratch_shapes=[pltpu.VMEM((rows, width), BF16), pltpu.VMEM((rows, cols), BF16), pltpu.VMEM((rows, width), BF16), pltpu.VMEM((rows, width), F32)],
        ),
        out_shape=[
            jax.ShapeDtypeStruct((layers, tiles, rows, cols), BF16),
            jax.ShapeDtypeStruct((layers, rows, width), BF16),
            jax.ShapeDtypeStruct((layers, width, kept_rows), BF16),
            jax.ShapeDtypeStruct((layers, tiles, 8, cols), F32),
            jax.ShapeDtypeStruct((8, width), F32),
        ],
        compiler_params=params(),
        cost_estimate=cost(4 * layers * rows * width * hidden, layers * hidden * (8 * width + 2 * rows), layers * rows * hidden),
        name="forward_now",
    )(tbl, x_rows, *([w_up] * SUBS), *([w_down] * SUBS))


def head_kernel(n_tok, n_all, positions, tbl, pool_ref, w_ref, lab_ref, hg_ref, g_ref, gt_ref, hg_s):
    n_img = 4
    width = pool_ref.shape[1]
    classes = w_ref.shape[0]
    pooled = (pool_ref[0:n_img, :] + pool_ref[n_img:8, :]) / n_tok
    pooled = jnp.concatenate([pooled, pooled], axis=0)
    w_b = w_ref[...].astype(BF16)
    normed = norm_rows(pooled).astype(BF16)
    logits = mm_t(normed, w_b)
    top = jnp.max(logits, axis=-1, keepdims=True)
    expd = jnp.exp(logits - top)
    probs = expd / jnp.sum(expd, axis=-1, keepdims=True)
    hit = lax.broadcasted_iota(I32, (8, classes), 1) == lab_ref[...]
    grad_logits = ((probs - jnp.where(hit, 1.0, 0.0)) / n_all).astype(BF16)
    once = jnp.where(lax.broadcasted_iota(I32, (8, classes), 0) < n_img, grad_logits.astype(F32), 0.0)
    once = jnp.concatenate([once, jnp.zeros((LANES - 8, classes), F32)], axis=0).astype(BF16)
    normed_t = transposed(normed, LANES)
    hg_s[...] = mm(normed_t, once)
    block = hg_ref.shape[1]
    for pos, rel in enumerate(positions):
        hg_ref[pos] = hg_s[pl.ds(pl.multiple_of(tbl[rel] * block, 8), block), :].astype(BF16)
    grad_normed = mm(grad_logits, w_b).astype(BF16)
    grad = (norm_grad(pooled, grad_normed.astype(F32)) / n_tok).astype(BF16)
    g_ref[...] = grad
    thrice = jnp.concatenate([jnp.where(lax.broadcasted_iota(I32, grad.shape, 0) < n_img, grad.astype(F32), 0.0)] * 3, axis=0)
    gt_ref[...] = transposed(thrice, LANES)


def head_now(tbl, pool, head_t, labels8, n_tok, n_all, n_dev):
    classes, width = head_t.shape
    order = ("c",) + HEAD_ORDER
    positions = []
    for pos in range(n_dev):
        rel = 0
        for k, name in enumerate(order):
            if (pos >> (len(order) - 1 - k)) & 1:
                rel |= MASK[name]
        positions.append(rel)
    block = width // n_dev
    vmem = pl.BlockSpec(memory_space=pltpu.VMEM)
    return pl.pallas_call(
        functools.partial(head_kernel, n_tok, n_all, tuple(positions)),
        in_specs=[pl.BlockSpec(memory_space=pltpu.SMEM), vmem, vmem, vmem],
        out_specs=[vmem, vmem, vmem],
        out_shape=[
            jax.ShapeDtypeStruct((n_dev, block, classes), BF16),
            jax.ShapeDtypeStruct((8, width), BF16),
            jax.ShapeDtypeStruct((width, LANES), BF16),
        ],
        scratch_shapes=[pltpu.VMEM((width, classes), F32)],
        compiler_params=params(),
        cost_estimate=cost(6 * 256 * width * classes, 8 * width * classes),
        name="head_now",
    )(tbl, pool, head_t, labels8)


def block_place(order, n_j_bits, last):
    n_axes = len(order)

    def bit_of(name, j):
        return {"y": j & 1, "z0": (j >> 1) & 1, "z1": (j >> 2) & 1}[name]

    shape = (2,) * n_axes + last
    block = tuple(2 if name == "x" else 1 for name in order) + last

    def index(j, t):
        return tuple(0 if name == "x" else bit_of(name, j) for name in order) + (0,) * len(last)

    def at(x):
        return tuple(x if name == "x" else 0 for name in order)

    return shape, block, index, at


def down_last_kernel(at, zs_ref, gt_ref, send_ref, keep_ref):
    zs = zs_ref[0, 0]
    n_img = 4
    zs = zs[0:n_img, :] + zs[n_img:8, :]
    high = zs.astype(BF16)
    rest = zs - high.astype(F32)
    mid = rest.astype(BF16)
    low = (rest - mid.astype(F32)).astype(BF16)
    zero4 = jnp.zeros((8 - n_img, zs.shape[1]), F32)
    parts = []
    for part in (high, mid, low):
        parts += [part.astype(F32), zero4]
    parts.append(jnp.zeros((LANES - 24, zs.shape[1]), F32))
    grad = mm(gt_ref[...], jnp.concatenate(parts, axis=0).astype(BF16)).astype(BF16)
    for i in range(SUBS):
        dst = keep_ref if i % 2 == 0 else send_ref
        dst[at(i // 2)] = grad[:, i * LANES : (i + 1) * LANES]


def down_last(zs, gp_t, order):
    layers, tiles, _, cols = zs.shape
    width = gp_t.shape[0]
    shape, block, index, at = block_place(order, 3, (width, LANES))
    return pl.pallas_call(
        functools.partial(down_last_kernel, at),
        grid=(tiles,),
        in_specs=[pl.BlockSpec((1, 1, 8, cols), lambda j: (layers - 1, j, 0, 0)), pl.BlockSpec((width, LANES), lambda j: (0, 0))],
        out_specs=[pl.BlockSpec(block, lambda j: index(j, None))] * 2,
        out_shape=[jax.ShapeDtypeStruct(shape, BF16)] * 2,
        compiler_params=params(),
        cost_estimate=cost(2 * 256 * width * tiles * cols, 2 * width * tiles * cols),
        name="down_last",
    )(zs, gp_t)


def finish_rows(valid, x_in, grad_rows, grad_u, g_ref, gt_ref):
    rows = x_in.shape[0]
    grad_norm = norm_grad(x_in.astype(F32), grad_u.astype(BF16).astype(F32))
    total = grad_rows.astype(F32) + grad_norm
    live = lax.broadcasted_iota(I32, (rows, 1), 0) < valid
    total = jnp.where(live, total, 0.0).astype(BF16)
    g_ref[...] = total
    gt_ref[...] = transposed(total, gt_ref.shape[1])


def up_last_kernel(at, valid, tbl, gp_ref, ut_ref, a_ref, x_ref, *refs):
    wd, wu = refs[0:4], refs[4:8]
    send_ref, keep_ref, g_ref, gt_ref, ga_s, acc = refs[8:]
    j = pl.program_id(0)
    rows, cols = a_ref.shape[2], a_ref.shape[3]

    @pl.when(j == 0)
    def _():
        acc[...] = jnp.zeros_like(acc)
        ga_s[...] = jnp.zeros_like(ga_s)

    grad_z = mm_t(gp_ref[...], side_by_side(wd, 0)).astype(BF16).astype(F32)
    _, slope = gelu_and_slope(a_ref[0, 0].astype(F32))
    grad_a = (slope.reshape(rows // 8, 8, cols) * grad_z[None]).reshape(rows, cols).astype(BF16)
    ga_s[0:rows, :] = grad_a
    grad = mm(ut_ref[0], ga_s[...]).astype(BF16)
    for i in range(SUBS):
        dst = keep_ref if i % 2 == 0 else send_ref
        dst[at(i // 2)] = grad[:, i * LANES : (i + 1) * LANES]
    acc[...] += mm_t(grad_a, side_by_side(wu, 1))

    @pl.when(j == pl.num_programs(0) - 1)
    def _():
        g_rows = gp_ref[...].astype(F32)
        g_rows = jnp.broadcast_to(g_rows[None], (rows // 8,) + g_rows.shape).reshape(rows, g_rows.shape[1])
        finish_rows(valid, x_ref[0], g_rows, acc[...], g_ref, gt_ref)


def up_last(tbl, gp, ut, a, xs, w_up, w_down, order, valid):
    layers, width, hidden = w_up.shape
    layer = layers - 1
    _, tiles, rows, cols = a.shape
    kept = ut.shape[2]
    shape, block, index, at = block_place(order, 3, (width, LANES))

    def up_spec(i):
        return pl.BlockSpec((1, width, LANES), lambda j, t: (layer, 0, t[j * SUBS + i]))

    def down_spec(i):
        return pl.BlockSpec((1, LANES, width), lambda j, t: (layer, t[j * SUBS + i], 0))

    return pl.pallas_call(
        functools.partial(up_last_kernel, at, valid),
        grid_spec=pltpu.PrefetchScalarGridSpec(
            num_scalar_prefetch=1,
            grid=(tiles,),
            in_specs=[
                pl.BlockSpec((8, width), lambda j, t: (0, 0)),
                pl.BlockSpec((1, width, kept), lambda j, t: (layer, 0, 0)),
                pl.BlockSpec((1, 1, rows, cols), lambda j, t: (layer, j, 0, 0)),
                pl.BlockSpec((1, rows, width), lambda j, t: (layer, 0, 0)),
            ]
            + [down_spec(i) for i in range(SUBS)]
            + [up_spec(i) for i in range(SUBS)],
            out_specs=[pl.BlockSpec(block, index)] * 2 + [pl.BlockSpec((rows, width), lambda j, t: (0, 0)), pl.BlockSpec((width, kept), lambda j, t: (0, 0))],
            scratch_shapes=[pltpu.VMEM((kept, cols), BF16), pltpu.VMEM((rows, width), F32)],
        ),
        out_shape=[jax.ShapeDtypeStruct(shape, BF16)] * 2 + [jax.ShapeDtypeStruct((rows, width), BF16), jax.ShapeDtypeStruct((width, kept), BF16)],
        compiler_params=params(),
        cost_estimate=cost(4.5 * rows * width * hidden, hidden * (8 * width + 2 * rows + 2 * width), rows * hidden),
        name="up_last",
    )(tbl, gp, ut, a, xs, *([w_down] * SUBS), *([w_up] * SUBS))


def block_grad_kernel(at, valid, want_u, first, last, tbl, g_ref, gt_ref, ut_ref, a_ref, *refs):
    refs = list(refs)
    wd = [refs.pop(0) for _ in range(SUBS)]
    wu = [refs.pop(0) for _ in range(SUBS)] if want_u else []
    acc_in = refs.pop(0) if want_u and not first else None
    x_ref = refs.pop(0) if want_u and last else None
    send_ref, keep_ref = refs.pop(0), refs.pop(0)
    acc_out = refs.pop(0) if want_u and not last else None
    g_out, gt_out = (refs.pop(0), refs.pop(0)) if want_u and last else (None, None)
    z_s, ga_s = refs.pop(0), refs.pop(0)
    acc = refs.pop(0) if want_u else None
    j = pl.program_id(0)
    rows = a_ref.shape[2]

    @pl.when(j == 0)
    def _():
        z_s[...] = jnp.zeros_like(z_s)
        ga_s[...] = jnp.zeros_like(ga_s)
        if want_u:
            acc[...] = jnp.zeros_like(acc) if first else acc_in[...]

    grad_z = mm_t(g_ref[...], side_by_side(wd, 0)).astype(BF16).astype(F32)
    z, slope = gelu_and_slope(a_ref[0, 0].astype(F32))
    z_s[0:rows, :] = z.astype(BF16)
    grad_a = (slope * grad_z).astype(BF16)
    ga_s[0:rows, :] = grad_a
    d_up = mm(ut_ref[0], ga_s[...]).astype(BF16)
    d_down = mm(gt_ref[...], z_s[...]).astype(BF16)
    for i in range(SUBS):
        dst = keep_ref if i % 2 == 0 else send_ref
        dst[at(i // 2) + (0,)] = d_up[:, i * LANES : (i + 1) * LANES]
        dst[at(i // 2) + (1,)] = d_down[:, i * LANES : (i + 1) * LANES]
    if want_u:
        acc[...] += mm_t(grad_a, side_by_side(wu, 1))

        @pl.when(j == pl.num_programs(0) - 1)
        def _():
            if last:
                finish_rows(valid, x_ref[0], g_ref[...], acc[...], g_out, gt_out)
            else:
                acc_out[...] = acc[...]


def block_grad(tbl, layer, half, g, g_t, ut, a, xs, acc_in, w_up, w_down, order, want_u, valid):
    layers, width, hidden = w_up.shape
    _, all_tiles, rows, cols = a.shape
    tiles = all_tiles // 2
    base = half * tiles
    kept = ut.shape[2]
    first, last = half == 1, half == 0
    shape, block, index, at = block_place(order, 2, (2, width, LANES))

    def up_spec(i):
        return pl.BlockSpec((1, width, LANES), lambda j, t: (layer, 0, t[(base + j) * SUBS + i]))

    def down_spec(i):
        return pl.BlockSpec((1, LANES, width), lambda j, t: (layer, t[(base + j) * SUBS + i], 0))

    whole = pl.BlockSpec((rows, width), lambda j, t: (0, 0))
    whole_t = pl.BlockSpec((width, kept), lambda j, t: (0, 0))
    args = [g, g_t, ut, a] + [w_down] * SUBS
    in_specs = [
        whole,
        whole_t,
        pl.BlockSpec((1, width, kept), lambda j, t: (layer, 0, 0)),
        pl.BlockSpec((1, 1, rows, cols), lambda j, t: (layer, base + j, 0, 0)),
    ] + [down_spec(i) for i in range(SUBS)]
    out_specs = [pl.BlockSpec(block, index)] * 2
    out_shape = [jax.ShapeDtypeStruct(shape, BF16)] * 2
    scratch = [pltpu.VMEM((kept, cols), BF16), pltpu.VMEM((kept, cols), BF16)]
    if want_u:
        args += [w_up] * SUBS
        in_specs += [up_spec(i) for i in range(SUBS)]
        scratch.append(pltpu.VMEM((rows, width), F32))
        if not first:
            args.append(acc_in)
            in_specs.append(whole)
        if last:
            args.append(xs)
            in_specs.append(pl.BlockSpec((1, rows, width), lambda j, t: (layer, 0, 0)))
            out_specs += [whole, whole_t]
            out_shape += [jax.ShapeDtypeStruct((rows, width), BF16), jax.ShapeDtypeStruct((width, kept), BF16)]
        else:
            out_specs.append(whole)
            out_shape.append(jax.ShapeDtypeStruct((rows, width), F32))
    return pl.pallas_call(
        functools.partial(block_grad_kernel, at, valid, want_u, first, last),
        grid_spec=pltpu.PrefetchScalarGridSpec(num_scalar_prefetch=1, grid=(tiles,), in_specs=in_specs, out_specs=out_specs, scratch_shapes=scratch),
        out_shape=out_shape,
        compiler_params=params(),
        cost_estimate=cost((8.5 if want_u else 6.5) / 2 * rows * width * hidden, hidden * (6 * width + rows), rows * hidden // 2),
        name=f"grad_{layer}_{half}",
    )(tbl, *args)


def exchange(values, name):
    size = lax.axis_size("data")
    return lax.ppermute(values, "data", [(i, i ^ MASK[name]) for i in range(size)])


def reduce_blocks(send, keep, order):
    got = exchange(send, "c")
    for name in order:
        send = keep[1] + got[1]
        keep = keep[0] + got[0]
        got = exchange(send, name)
    return keep, got


def gather_blocks(block, sub):
    have = block
    for k, name in enumerate(GATHER_FIRST[sub]):
        got = exchange(have, name)
        have = jnp.stack([have, got])
    far = exchange(have, sub)
    return [have, exchange(have, "c"), far, exchange(far, "c")]


def sub_place(sub):
    def position(j, i):
        far, core = (i >> 1), (i & 1)
        if sub == "x":
            return j * 4 + far * 2 + core
        if sub == "y":
            return (j >> 1) * 8 + far * 4 + (j & 1) * 2 + core
        return (j >> 2) * 16 + far * 8 + (j & 3) * 2 + core

    def tile(j):
        return (j & 1, (j >> 1) & 1, j >> 2, 0, 0)

    def z_block(rows):
        return tuple(2 if name in (sub, "c") else 1 for name in ("z1", "z0", "y", "x", "c")) + (rows, LANES)

    def z_index(j):
        bits = {"x": (j >> 2, (j >> 1) & 1, j & 1, 0), "y": (j >> 2, (j >> 1) & 1, 0, j & 1), "z0": (j >> 2, 0, (j >> 1) & 1, j & 1)}[sub]
        return bits + (0, 0, 0)

    def z_at(i):
        pos = {"x": (0, 0, 0, i >> 1), "y": (0, 0, i >> 1, 0), "z0": (0, i >> 1, 0, 0)}[sub]
        return pos + (i & 1,)

    return position, tile, z_block, z_index, z_at


def send_tile(copies, j, last):
    slot = lax.rem(j, 2)
    for copy in copies(slot, j):
        copy.start()

    @pl.when(j == last)
    def _():
        for copy in copies(slot, j):
            copy.wait()

        @pl.when(j >= 1)
        def _():
            for copy in copies(1 - slot, j - 1):
                copy.wait()


def free_slot(copies, j):
    @pl.when(j >= 2)
    def _():
        for copy in copies(lax.rem(j, 2), j - 2):
            copy.wait()


def next_up_kernel(layer, position, z_at, aliased, tbl, rate, x_ref, *refs):
    refs = list(refs)
    w = [refs.pop(0) for _ in range(SUBS)]
    p = [refs.pop(0) for _ in range(SUBS)]
    if aliased:
        refs.pop(0)
    new_w, z_ref, u_s, w_s, sem = refs
    j = pl.program_id(0)
    last = pl.num_programs(0) - 1

    def copies(slot, jj):
        out = []
        for i in range(SUBS):
            start = pl.multiple_of(tbl[position(jj, i)] * LANES, LANES)
            out.append(pltpu.make_async_copy(w_s.at[slot, i], new_w.at[layer, :, pl.ds(start, LANES)], sem.at[slot, i]))
        return out

    @pl.when(j == 0)
    def _():
        u_s[...] = norm_rows(x_ref[...].astype(F32)).astype(BF16)

    free_slot(copies, j)
    slot = lax.rem(j, 2)
    parts = []
    for i in range(SUBS):
        fresh = w[i][0] - rate[0] * p[i][0, 0, 0].astype(F32)
        w_s[slot, i] = fresh
        parts.append(fresh.astype(BF16))
    send_tile(copies, j, last)
    a = mm(u_s[...], jnp.concatenate(parts, axis=1)).astype(BF16)
    z = gelu(a.astype(F32)).astype(BF16)
    for i in range(SUBS):
        z_ref[z_at(i)] = z[:, i * LANES : (i + 1) * LANES]


def next_down_kernel(layer, position, z_at, aliased, pool, tbl, rate, x_ref, z_ref, *refs):
    refs = list(refs)
    w = [refs.pop(0) for _ in range(SUBS)]
    p = [refs.pop(0) for _ in range(SUBS)]
    if aliased:
        refs.pop(0)
    new_w, x_out, w_s, acc, sem = refs
    j = pl.program_id(0)
    last = pl.num_programs(0) - 1

    def copies(slot, jj):
        out = []
        for i in range(SUBS):
            start = pl.multiple_of(tbl[position(jj, i)] * LANES, LANES)
            out.append(pltpu.make_async_copy(w_s.at[slot, i], new_w.at[layer, pl.ds(start, LANES), :], sem.at[slot, i]))
        return out

    @pl.when(j == 0)
    def _():
        acc[...] = jnp.zeros_like(acc)

    free_slot(copies, j)
    slot = lax.rem(j, 2)
    parts = []
    for i in range(SUBS):
        fresh = w[i][0] - rate[0] * p[i][0, 0, 0].astype(F32)
        w_s[slot, i] = fresh
        parts.append(fresh.astype(BF16))
    send_tile(copies, j, last)
    z = jnp.concatenate([z_ref[z_at(i)] for i in range(SUBS)], axis=1)
    acc[...] += mm(z, jnp.concatenate(parts, axis=0))

    @pl.when(j == last)
    def _():
        y = acc[...].astype(BF16)
        x_new = (x_ref[...].astype(F32) + y.astype(F32)).astype(BF16)
        if pool:
            x_out[...] = fold_rows(x_new.astype(F32))
        else:
            x_out[...] = x_new


def next_up(tbl, rate, layer, x_rows, w_up, gathered, sub, new_w):
    layers, width, hidden = w_up.shape
    rows = x_rows.shape[0]
    tiles = hidden // (LANES * SUBS)
    position, tile, z_block, z_index, z_at = sub_place(sub)
    aliased = new_w is not None

    def w_spec(i):
        return pl.BlockSpec((1, width, LANES), lambda j, t: (layer, 0, t[position(j, i)]))

    in_specs = [pl.BlockSpec(memory_space=pltpu.SMEM), pl.BlockSpec((rows, width), lambda j, t: (0, 0))]
    in_specs += [w_spec(i) for i in range(SUBS)] + [pl.BlockSpec((1, 1, 1, width, LANES), lambda j, t: tile(j))] * SUBS
    args = [rate, x_rows] + [w_up] * SUBS + gathered
    if aliased:
        in_specs.append(pl.BlockSpec(memory_space=pl.ANY))
        args.append(new_w)
    return pl.pallas_call(
        functools.partial(next_up_kernel, layer, position, z_at, aliased),
        grid_spec=pltpu.PrefetchScalarGridSpec(
            num_scalar_prefetch=1,
            grid=(tiles,),
            in_specs=in_specs,
            out_specs=[pl.BlockSpec(memory_space=pl.ANY), pl.BlockSpec(z_block(rows), lambda j, t: z_index(j))],
            scratch_shapes=[pltpu.VMEM((rows, width), BF16), pltpu.VMEM((2, SUBS, width, LANES), F32), pltpu.SemaphoreType.DMA((2, SUBS))],
        ),
        out_shape=[jax.ShapeDtypeStruct(w_up.shape, F32), jax.ShapeDtypeStruct((2,) * 5 + (rows, LANES), BF16)],
        input_output_aliases={len(args): 0} if aliased else {},
        compiler_params=params(),
        cost_estimate=cost(2 * rows * width * hidden, hidden * (10 * width + 2 * rows), rows * hidden),
        name=f"next_up_{layer}",
    )(tbl, *args)


def next_down(tbl, rate, layer, x_rows, z, w_down, gathered, sub, new_w, pool):
    layers, hidden, width = w_down.shape
    rows = x_rows.shape[0]
    tiles = hidden // (LANES * SUBS)
    position, tile, z_block, z_index, z_at = sub_place(sub)
    aliased = new_w is not None

    def w_spec(i):
        return pl.BlockSpec((1, LANES, width), lambda j, t: (layer, t[position(j, i)], 0))

    in_specs = [
        pl.BlockSpec(memory_space=pltpu.SMEM),
        pl.BlockSpec((rows, width), lambda j, t: (0, 0)),
        pl.BlockSpec(z_block(rows), lambda j, t: z_index(j)),
    ]
    in_specs += [w_spec(i) for i in range(SUBS)] + [pl.BlockSpec((1, 1, 1, LANES, width), lambda j, t: tile(j))] * SUBS
    args = [rate, x_rows, z] + [w_down] * SUBS + gathered
    if aliased:
        in_specs.append(pl.BlockSpec(memory_space=pl.ANY))
        args.append(new_w)
    out_rows, out_type = (8, F32) if pool else (rows, BF16)
    return pl.pallas_call(
        functools.partial(next_down_kernel, layer, position, z_at, aliased, pool),
        grid_spec=pltpu.PrefetchScalarGridSpec(
            num_scalar_prefetch=1,
            grid=(tiles,),
            in_specs=in_specs,
            out_specs=[pl.BlockSpec(memory_space=pl.ANY), pl.BlockSpec((out_rows, width), lambda j, t: (0, 0))],
            scratch_shapes=[pltpu.VMEM((2, SUBS, LANES, width), F32), pltpu.VMEM((rows, width), F32), pltpu.SemaphoreType.DMA((2, SUBS))],
        ),
        out_shape=[jax.ShapeDtypeStruct(w_down.shape, F32), jax.ShapeDtypeStruct((out_rows, width), out_type)],
        input_output_aliases={len(args): 0} if aliased else {},
        compiler_params=params(),
        cost_estimate=cost(2 * rows * width * hidden, hidden * (10 * width + 2 * rows)),
        name=f"next_down_{layer}",
    )(tbl, *args)


def head_update_kernel(position, tbl, rate, w_ref, p0, p1, p2, p3, new_ref, cast_ref, m_s):
    block = p0.shape[3]
    for j in range(8):
        for i, part in enumerate((p0, p1, p2, p3)):
            rows = part[j & 1, (j >> 1) & 1, j >> 2].astype(F32)
            m_s[pl.ds(pl.multiple_of(tbl[position(j, i)] * block, 8), block), 0 : rows.shape[1]] = rows
    classes = w_ref.shape[0]
    fresh = w_ref[...] - rate[0] * m_s[...].T[0:classes, :]
    new_ref[...] = fresh
    cast_ref[...] = fresh.astype(BF16)


def head_update(tbl, rate, head_t, gathered, sub):
    classes, width = head_t.shape
    position = sub_place(sub)[0]
    vmem, smem = pl.BlockSpec(memory_space=pltpu.VMEM), pl.BlockSpec(memory_space=pltpu.SMEM)
    padded = (classes + LANES - 1) // LANES * LANES
    return pl.pallas_call(
        functools.partial(head_update_kernel, position),
        in_specs=[smem, smem] + [vmem] * 5,
        out_specs=[vmem, vmem],
        out_shape=[jax.ShapeDtypeStruct((classes, width), F32), jax.ShapeDtypeStruct((classes, width), BF16)],
        scratch_shapes=[pltpu.VMEM((width, padded), F32)],
        compiler_params=params(),
        cost_estimate=cost(2 * width * classes, 12 * width * classes),
        name="head_update",
    )(tbl, rate, head_t, *gathered)


def head_next_kernel(n_tok, pool_ref, w_ref, out_ref):
    n_img = out_ref.shape[0]
    pooled = (pool_ref[0:n_img, :] + pool_ref[n_img : 2 * n_img, :]) / n_tok
    pooled = jnp.concatenate([pooled, pooled], axis=0)
    out_ref[...] = mm_t(norm_rows(pooled).astype(BF16), w_ref[...])[0:n_img, :]


def head_next(pool, head_b, n_img, n_tok):
    vmem = pl.BlockSpec(memory_space=pltpu.VMEM)
    return pl.pallas_call(
        functools.partial(head_next_kernel, n_tok),
        in_specs=[vmem, vmem],
        out_specs=vmem,
        out_shape=jax.ShapeDtypeStruct((n_img, head_b.shape[0]), F32),
        compiler_params=params(),
        cost_estimate=cost(512 * head_b.shape[0] * head_b.shape[1], 2 * head_b.size),
        name="head_next",
    )(pool, head_b)


def to_rows(x_in, rows):
    n_img, n_tok, width = x_in.shape
    flat = jnp.transpose(x_in, (1, 0, 2)).reshape(n_tok * n_img, width)
    return jnp.pad(flat, ((0, rows - n_tok * n_img), (0, 0)))


def solution(mesh):
    n_dev = mesh.shape["data"]

    def local_step(x_now, x_next, labels, w_up, w_down, w_head, mom_up, mom_down, mom_head, learn_rate, mom_decay):
        n_img, n_tok, width = x_now.shape
        valid = n_img * n_tok
        rows = (valid + 15) // 16 * 16
        kept_rows = (rows + LANES - 1) // LANES * LANES
        tbl = lax.axis_index("data").astype(I32) ^ jnp.arange(n_dev, dtype=I32)
        rate = learn_rate.reshape(1)
        labels8 = jnp.tile(labels, 8 // n_img).reshape(8, 1)
        head_t = w_head.T

        a, xs, ut, zs, pool = forward_now(tbl, to_rows(x_now, rows), w_up, w_down, kept_rows)
        head_grad, gp, gp_t = head_now(tbl, pool, head_t, labels8, n_tok, n_img * n_dev, n_dev)

        send, keep = down_last(zs, gp_t, DOWN_LAST)
        down2 = reduce_blocks(send, keep, DOWN_LAST)
        send, keep, g, g_t = up_last(tbl, gp, ut, a, xs, w_up, w_down, UP_LAST, valid)
        up2 = reduce_blocks(send, keep, UP_LAST)
        half = n_dev // 2
        head_grad = head_grad.reshape((2,) * 5 + head_grad.shape[1:])
        head_sum = reduce_blocks(head_grad[1], head_grad[0], HEAD_ORDER)

        up_sums, down_sums = [None] * 3, [None] * 3
        up_sums[2] = up2[0].astype(F32) + up2[1].astype(F32)
        down_sums[2] = down2[0].astype(F32) + down2[1].astype(F32)
        for layer in (1, 0):
            want_u = layer > 0
            order = HALF_ORDERS[layer, 1]
            out = block_grad(tbl, layer, 1, g, g_t, ut, a, xs, None, w_up, w_down, order, want_u, valid)
            far = reduce_blocks(out[0], out[1], order)
            order = HALF_ORDERS[layer, 0]
            out2 = block_grad(tbl, layer, 0, g, g_t, ut, a, xs, out[2] if want_u else None, w_up, w_down, order, want_u, valid)
            if want_u:
                g, g_t = out2[2], out2[3]
            near = reduce_blocks(out2[0], out2[1], order)
            got = exchange(far[0] + far[1], "z1")
            total = (near[0].astype(F32) + near[1].astype(F32)) + got.astype(F32)
            up_sums[layer], down_sums[layer] = total[0], total[1]

        new_up = [mom_decay * mom_up[l] + up_sums[l] for l in range(3)]
        new_down = [mom_decay * mom_down[l] + down_sums[l].T for l in range(3)]
        new_head = mom_decay * mom_head + (head_sum[0].astype(F32) + head_sum[1].astype(F32))

        gathered_head = gather_blocks(new_head.astype(BF16), "x")
        x_rows = to_rows(x_next, rows)
        new_w_up = new_w_down = None
        for layer in range(3):
            sub = GATHER_SUB["up", layer]
            parts = gather_blocks(new_up[layer].astype(BF16), sub)
            new_w_up, z = next_up(tbl, rate, layer, x_rows, w_up, parts, sub, new_w_up)
            sub = GATHER_SUB["down", layer]
            parts = gather_blocks(new_down[layer].astype(BF16), sub)
            new_w_down, x_rows = next_down(tbl, rate, layer, x_rows, z, w_down, parts, sub, new_w_down, layer == 2)
        new_head_t, head_b = head_update(tbl, rate, head_t, gathered_head, "x")
        logits_next = head_next(x_rows, head_b, n_img, n_tok)
        return (logits_next, new_w_up, new_w_down, new_head_t.T, jnp.stack(new_up), jnp.stack(new_down), new_head)

    spec_up = P(None, None, "data")
    spec_down = P(None, "data", None)
    spec_head = P("data", None)
    return jax.shard_map(
        local_step,
        mesh=mesh,
        in_specs=(P("data"), P("data"), P("data"), P(), P(), P(), spec_up, spec_down, spec_head, P(), P()),
        out_specs=(P("data"), P(), P(), P(), spec_up, spec_down, spec_head),
        check_vma=False,
    )
```
